32 devices in a mesh: leaf: 8 (over z, x), cols: 4 (over y, core).
Axes of the slice: x: 2, y: 2, z: 4, core: 2. Of those that a mesh axis runs over, the one named last changes fastest.
Arguments:
- samples: bfloat16 [2048, 16384], P('cols', 'leaf'), may hold values from -6 to 6
- order_perm: int32 [16384], P('leaf'), may hold values from 0 to 16383, as said below
- leaf_factor: bfloat16 [16, 1024, 1024], P('leaf'), may hold values from -0.1875 to 0.1875
- bases: bfloat16 [4, 64, 16384], P(None, None, 'leaf'), may hold values from -110 to 110
- coupling: float32 [4, 8, 64, 64], P(None, 'leaf'), may hold values from -1 to 1, as said below
- ranks: int32 [4, 16], replicated, may hold values from 16 to 64
Outputs:
- transformed: float32 [2048, 16384], P('cols', 'leaf')
The draws below stay inside these ranges and needn't reach their ends.
Inputs may be any that keep to these rules, and one draw needn't show every extreme that they name: `order_perm`: each aligned block of 2048 positions holds a permutation of the same block's indices. coupling[l, d] equals coupling[l, e] whenever d and e lie in the same level-l node, that is d // 2**l == e // 2**l.
All inputs are finite; a program needn't handle non-finite values.
Results may differ from the reference program's by a relative error of at most 0.0003.
Values sent between devices are 32-bit elements; how exact they have to be, the bound alone decides.
A program may use at most 128 MiB of HBM per device.

```python
import jax
import jax.numpy as jnp
from jax import lax

LEAF = 1024
R = 64
ROWS_DEV = 2048
ORDER = 16384
NLEAVES = 16
NCOLS = 2048
LEVELS = 4


def draw_order_perm(key, part):
    devices = ORDER // ROWS_DEV
    keys = jax.random.split(jax.random.fold_in(key, 11), devices)
    perms = jax.vmap(lambda one_key: jax.random.permutation(one_key, ROWS_DEV))(keys)
    offsets = jnp.arange(devices, dtype=jnp.int32)[:, None] * ROWS_DEV
    return (perms.astype(jnp.int32) + offsets).reshape(-1).astype(jnp.int32)


def draw_coupling(key, part):
    devices = ORDER // ROWS_DEV
    inner_key = jax.random.fold_in(key, 23)
    base = jax.random.normal(inner_key, (LEVELS, devices, R, R), jnp.float32) / R ** 0.5
    base = jnp.clip(base, -1.0, 1.0)
    shifts = jnp.arange(LEVELS, dtype=jnp.int32)[:, None]
    source = jnp.arange(devices, dtype=jnp.int32)[None, :] >> shifts << shifts
    picked = jax.vmap(lambda level_base, level_source: level_base[level_source])(base, source)
    return picked.astype(jnp.float32)


def draw_bases(key, part):
    devices = ORDER // ROWS_DEV
    entry_key = jax.random.fold_in(key, 31)
    factor_key = jax.random.fold_in(key, 37)
    position = jnp.arange(devices, dtype=jnp.float32) / max(devices - 1, 1)
    entries = jnp.clip(jax.random.normal(entry_key, (LEVELS, R, devices, ROWS_DEV), jnp.float32), -6.0, 6.0)
    rising = 3.0 ** position
    factors = jax.random.uniform(factor_key, (LEVELS, 1, devices, 1), jnp.float32, 1.0, 2.0)
    scaled = entries * factors * rising[None, None, :, None]
    return scaled.reshape(LEVELS, R, ORDER).astype(jnp.bfloat16)


def touch_ends(values, rng, smallest, high):
    spot = [jax.random.randint(jax.random.fold_in(rng, axis), (), 0, length) for axis, length in enumerate(values.shape)]
    main_axis = values.shape.index(max(values.shape))
    neighbour = spot[:main_axis] + [(spot[main_axis] + 1) % values.shape[main_axis]] + spot[main_axis + 1:]
    return values.at[tuple(spot)].set(smallest).at[tuple(neighbour)].set(high)


def shard_levels(rng, shape, shards, low, top_value):
    def one(axis_at, shards_of):
        steps = jax.random.uniform(jax.random.fold_in(jax.random.fold_in(rng, 6), axis_at), (shards_of,), jnp.float32, low / len(shards), top_value / len(shards))
        return jnp.repeat(jnp.exp(steps), shape[axis_at] // shards_of).reshape((-1,) + (1,) * (len(shape) - axis_at - 1))

    loudness = one(*shards[0])
    for cut in shards[1:]:
        loudness = loudness * one(*cut)
    return loudness


def normal_values(own_key, extent, scale, most, shards=(), kind=jnp.bfloat16):
    factor_of = shard_levels(own_key, extent, shards, -0.22, 0.18) if shards else 1.0
    drawn = jax.random.normal(own_key, extent, jnp.float32) * scale * factor_of
    return jnp.minimum(jnp.maximum(drawn, -most), most).astype(kind)


def setup_inputs(seed: int = 0) -> dict:
    seeds = jax.random.split(jax.random.key(seed), 7)
    samples = normal_values(seeds[0], (NCOLS, ORDER), 1.0, 6.0, ((0, 4), (1, 8)))
    order_perm = draw_order_perm(jax.random.fold_in(seeds[6], 71), 0)
    leaf_factor = normal_values(seeds[2], (NLEAVES, LEAF, LEAF), LEAF ** -0.5, 0.1875, ((0, 8),))
    bases = draw_bases(jax.random.fold_in(seeds[6], 71), 0)
    coupling = draw_coupling(jax.random.fold_in(seeds[6], 71), 0)
    ranks = touch_ends(jax.random.randint(seeds[5], (LEVELS, NLEAVES), R // 4, R + 1), jax.random.fold_in(seeds[5], 1), R // 4, R).astype(jnp.int32)
    return dict(samples=samples, order_perm=order_perm, leaf_factor=leaf_factor, bases=bases, coupling=coupling, ranks=ranks)


HIGH = lax.Precision.HIGHEST

def chol_apply(system, right_side):
    lower_factor = jnp.linalg.cholesky(system)
    middle = lax.linalg.triangular_solve(lower_factor, right_side, left_side=True, lower=True)
    return lax.linalg.triangular_solve(lower_factor, middle, left_side=True, lower=True, transpose_a=True)

def coupled(coupling_now, gram_other, proj_other):
    rank_width = coupling_now.shape[-1]
    inner = jnp.matmul(coupling_now, gram_other, precision=HIGH)
    system = jnp.eye(rank_width, dtype=jnp.float32) + jnp.matmul(inner, jnp.swapaxes(coupling_now, -1, -2), precision=HIGH)
    return chol_apply(system, jnp.matmul(coupling_now, proj_other, precision=HIGH))

def leaf_product(leaf_pair):
    return jnp.dot(leaf_pair[0].astype(jnp.float32), leaf_pair[1].astype(jnp.float32), preferred_element_type=jnp.float32)

def reference(samples, order_perm, leaf_factor, bases, coupling, ranks):
    permuted = jnp.take(samples, order_perm, axis=1)
    blocks = jnp.swapaxes(permuted.reshape(NCOLS, NLEAVES, LEAF), 0, 1)
    leaf_out = lax.map(leaf_product, (blocks, leaf_factor))
    field = jnp.swapaxes(leaf_out, 0, 1).reshape(NCOLS, ORDER)
    for tree_level in range(LEVELS):
        child_rows = LEAF * 2 ** tree_level
        nodes = ORDER // (2 * child_rows)
        scale = 1.0 / child_rows ** 0.5
        state = field.reshape(NCOLS, nodes, 2, child_rows)
        ranks_here = ranks[tree_level, ::2 ** tree_level].reshape(nodes, 2)
        column_mask = (jnp.arange(R, dtype=jnp.int32)[None, None, :] < ranks_here[:, :, None]).astype(jnp.float32) * scale
        basis = bases[tree_level].astype(jnp.float32).reshape(R, nodes, 2, child_rows)
        basis = basis * jnp.transpose(column_mask, (2, 0, 1))[..., None]
        proj = jnp.einsum('rmkc,jmkc->mkrj', basis, state, precision=HIGH)
        gram = jnp.einsum('rmkc,smkc->mkrs', basis, basis, precision=HIGH)
        links = coupling[tree_level, ::2 ** tree_level]
        first_update = coupled(links, gram[:, 1], proj[:, 1])
        second_update = coupled(jnp.swapaxes(links, -1, -2), gram[:, 0], proj[:, 0])
        updates = jnp.stack([first_update, second_update], axis=1)
        state = state - jnp.einsum('mkrj,rmkc->jmkc', updates, basis, precision=HIGH)
        field = state.reshape(NCOLS, ORDER)
    return field
```

```python
import functools
import math

import jax
import jax.numpy as jnp
from jax import lax
from jax.experimental import pallas as pl
from jax.experimental.pallas import tpu as pltpu
from jax.sharding import PartitionSpec as P

HIGH = lax.Precision.HIGHEST
MIB = 1024 * 1024
BLOCK = 256


def dot_high(a, b, contract=((1,), (0,))):
    return lax.dot_general(
        a, b, (contract, ((), ())), precision=HIGH, preferred_element_type=jnp.float32
    )


def dot_bf16(a, b, contract=((1,), (0,))):
    return lax.dot_general(a, b, (contract, ((), ())), preferred_element_type=jnp.float32)


def split(values):
    high = values.astype(jnp.bfloat16)
    return high, (values - high.astype(jnp.float32)).astype(jnp.bfloat16)


def mask(rank_value, rank_width, scale, axis):
    shape = (1, rank_width) if axis else (rank_width, 1)
    return jnp.where(lax.broadcasted_iota(jnp.int32, shape, axis) < rank_value, scale, 0.0)


def place_system(table, slot, link, gram):
    width = link.shape[0]
    rows = lax.broadcasted_iota(jnp.int32, (width, width), 0)
    eye = (rows == lax.broadcasted_iota(jnp.int32, (width, width), 1)).astype(jnp.float32)
    system = eye + dot_high(dot_high(link, gram), link, ((1,), (1,)))
    table[slot, :, :width] = system
    table[slot, :, width:] = link


def eliminate(table, slots, pivot):
    width, span = table.shape[1:]
    lanes = lax.broadcasted_iota(jnp.int32, (width, span), 1)
    rows = lax.broadcasted_iota(jnp.int32, (width, span), 0)
    for slot in slots:
        now = table[slot]
        row = table[slot, pl.ds(pivot, 1), :]
        column = jnp.sum(jnp.where(lanes == pivot, now, 0.0), axis=1, keepdims=True)
        top = jnp.sum(jnp.where(lanes[:1] == pivot, row, 0.0), axis=1, keepdims=True)
        row = row / top
        table[slot] = jnp.where(rows == pivot, row, now - column * row)


def pair_order(levels):
    return [(l, m) for m in range(1, levels) for l in range(m, levels)]


def local_kernel(levels, width, ranks, samples, order, basis, coupling, leaf_hbm,
                 permuted, proj_out, first_out, gram_out, leaf, table, grams, weights, sem):
    device = lax.axis_index("leaf")
    row_count = samples.shape[1]
    half = row_count // 2
    fetch = pltpu.make_async_copy(leaf_hbm, leaf, sem)
    fetch.start()
    for side in range(2):
        part = basis[:, side * half:(side + 1) * half]
        grams[side] = dot_bf16(part, part, ((1,), (1,)))
    for index, (l, m) in enumerate(pair_order(levels)):
        rows, cols = pl.ds(l * width, width), pl.ds(m * width, width)
        gram_out[index // 2, :, pl.ds(index % 2 * width, width)] = (
            grams[0, rows, cols] + grams[1, rows, cols]
        )
    scale = 1.0 / math.sqrt(half)
    rank = [ranks[0, 2 * device], ranks[0, 2 * device + 1]]
    link = coupling[0, 0]
    links = [link, link.T]
    for side in range(2):
        scaled = links[side] * mask(rank[1 - side], width, scale, 1)
        place_system(table, side, scaled, grams[1 - side, :width, :width])

    blocks = row_count // BLOCK
    per_block = width // blocks

    def permute(block, carry):
        cols = pl.ds(pl.multiple_of(block * BLOCK, BLOCK), BLOCK)
        source = order[:, cols] - device * row_count
        picks = lax.broadcasted_iota(jnp.int32, (row_count, BLOCK), 0) == source
        picks = picks.astype(jnp.float32).astype(jnp.bfloat16)
        permuted[:, cols] = dot_bf16(samples[...], picks).astype(jnp.bfloat16)
        for step in range(per_block):
            eliminate(table, range(2), block * per_block + step)
        return carry

    lax.fori_loop(0, blocks, permute, 0)
    fetch.wait()
    height = levels * width
    projs = []
    for side in range(2):
        cols = slice(side * half, (side + 1) * half)
        high, low = split(dot_bf16(basis[:, cols], leaf[side], ((1,), (1,))))
        weights[:height] = high
        weights[height:] = low
        both = dot_bf16(weights[...], permuted[:, cols], ((1,), (1,)))
        projs.append(both[:height] + both[height:])
    later = projs[0][width:] + projs[1][width:]
    for side in range(2):
        solved = table[side, :, width:] * mask(rank[side], width, scale, 0)
        update = dot_high(solved, projs[1 - side][:width])
        first_out[side] = update
        later = later - dot_high(grams[side, width:, :width], update)
    chunks, _, chunk = proj_out.shape
    for index in range(chunks):
        proj_out[index] = later[:, index * chunk:(index + 1) * chunk]


def tree_kernel(levels, width, leaf_rows, ranks, grams, proj, coupling, update_out,
                gram_sum, gram_recv, proj_sum, proj_recv, table,
                gram_send_sem, gram_recv_sem, proj_send_sem, proj_recv_sem):
    device = lax.axis_index("leaf")
    steps = levels - 1
    chunks, _, chunk = proj.shape
    order = pair_order(levels)
    pairs = grams.shape[0]

    def partner(step):
        stride = 2 ** (step - 1)
        return device + stride * (1 - 2 * (device // stride % 2))

    barrier = pltpu.get_barrier_semaphore()
    for step in range(1, levels):
        pl.semaphore_signal(
            barrier, inc=1, device_id={"leaf": partner(step)},
            device_id_type=pl.DeviceIdType.MESH,
        )
    pl.semaphore_wait(barrier, steps)

    def gram_own(step):
        return grams if step == 1 else gram_sum.at[step - 2]

    def proj_own(step, index):
        return proj.at[index] if step == 1 else proj_sum.at[step - 2, index]

    def send_gram(step):
        first = order.index((step, step)) // 2
        kept = pl.ds(first, pairs - first)
        return pltpu.make_async_remote_copy(
            src_ref=gram_own(step).at[kept],
            dst_ref=gram_recv.at[step - 1, kept],
            send_sem=gram_send_sem.at[step - 1],
            recv_sem=gram_recv_sem.at[step - 1],
            device_id={"leaf": partner(step)},
            device_id_type=pl.DeviceIdType.MESH,
        )

    def send_proj(step, index):
        kept = pl.ds((step - 1) * width, (levels - step) * width)
        return pltpu.make_async_remote_copy(
            src_ref=proj_own(step, index).at[kept],
            dst_ref=proj_recv.at[step - 1, index, kept],
            send_sem=proj_send_sem.at[step - 1, index],
            recv_sem=proj_recv_sem.at[step - 1, index],
            device_id={"leaf": partner(step)},
            device_id_type=pl.DeviceIdType.MESH,
        )

    def block(ref, pair):
        index = order.index(pair)
        return ref[index // 2, :, pl.ds(index % 2 * width, width)]

    gram_copies = [send_gram(1)]
    gram_copies[0].start()
    proj_copies = {}
    for index in range(chunks):
        proj_copies[1, index] = send_proj(1, index)
        proj_copies[1, index].start()
    masks = {}
    for step in range(1, levels):
        gram_copies[step - 1].wait_recv()
        first = order.index((step, step)) // 2
        if step < steps:
            kept = pl.ds(first, pairs - first)
            gram_sum[step - 1, kept] = gram_own(step)[kept] + gram_recv[step - 1, kept]
            gram_copies.append(send_gram(step + 1))
            gram_copies[step].start()
        scale = 1.0 / math.sqrt(leaf_rows * 2 ** step)
        stride = 2 ** (step - 1)
        child = device // stride
        second = child % 2
        sibling = child + 1 - 2 * second
        rank_own = ranks[step, child * 2 ** step]
        rank_other = ranks[step, sibling * 2 ** step]
        masks[step] = (mask(rank_own, width, scale, 0), mask(rank_other, width, scale, 0))
        link = coupling[step, 0]
        link_own = jnp.where(second == 1, link.T, link)
        scaled = link_own * mask(rank_other, width, scale, 1)
        place_system(table, 2 * step - 2, scaled, block(gram_recv.at[step - 1], (step, step)))
        if step < steps:
            scaled = link_own.T * mask(rank_own, width, scale, 1)
            place_system(table, 2 * step - 1, scaled, block(gram_own(step), (step, step)))

    def pivot_step(pivot, carry):
        eliminate(table, range(2 * steps - 1), pivot)
        return carry

    lax.fori_loop(0, width, pivot_step, 0)

    for step in range(1, levels):
        base = (step - 1) * width
        solved_own = table[2 * step - 2, :, width:] * masks[step][0]
        if step < steps:
            solved_other = table[2 * step - 1, :, width:] * masks[step][1]
        for index in range(chunks):
            proj_copies[step, index].wait_recv()
            mine, other = proj_own(step, index), proj_recv.at[step - 1, index]
            update_own = dot_high(solved_own, other[pl.ds(base, width)])
            update_out[pl.ds(base, width), pl.ds(index * chunk, chunk)] = update_own
            if step == steps:
                continue
            update_other = dot_high(solved_other, mine[pl.ds(base, width)])
            for level in range(step + 1, levels):
                rows = pl.ds((level - 1) * width, width)
                new = mine[rows] + other[rows]
                new = new - dot_high(block(gram_own(step), (level, step)), update_own)
                new = new - dot_high(
                    block(gram_recv.at[step - 1], (level, step)), update_other
                )
                proj_sum[step - 1, index, rows] = new
            proj_copies[step + 1, index] = send_proj(step + 1, index)
            proj_copies[step + 1, index].start()
    for copy in gram_copies + list(proj_copies.values()):
        copy.wait_send()


def final_kernel(permuted, leaf, basis, first, later, out):
    update = jnp.concatenate([first[0], later[...]], axis=0)
    high, low = split(update)
    field = dot_bf16(permuted[...], leaf[0])
    field = field - dot_bf16(high, basis[...], ((0,), (0,)))
    out[...] = field - dot_bf16(low, basis[...], ((0,), (0,)))


def local(samples, order_perm, leaf_factor, bases, coupling, ranks):
    cols, row_count = samples.shape
    levels, width, _ = bases.shape
    leaf_rows = leaf_factor.shape[1]
    steps = levels - 1
    basis = bases.reshape(levels * width, row_count)
    pairs = (len(pair_order(levels)) + 1) // 2
    chunks = 2
    chunk = cols // chunks
    vmem = pl.BlockSpec(memory_space=pltpu.VMEM)
    smem = pl.BlockSpec(memory_space=pltpu.SMEM)
    f32 = jnp.float32
    permuted, proj, first, grams = pl.pallas_call(
        functools.partial(local_kernel, levels, width),
        name="local_part",
        out_shape=(
            jax.ShapeDtypeStruct((cols, row_count), jnp.bfloat16),
            jax.ShapeDtypeStruct((chunks, steps * width, chunk), f32),
            jax.ShapeDtypeStruct((2, width, cols), f32),
            jax.ShapeDtypeStruct((pairs, width, 2 * width), f32),
        ),
        in_specs=[smem, vmem, vmem, vmem, vmem, pl.BlockSpec(memory_space=pl.ANY)],
        out_specs=(vmem,) * 4,
        scratch_shapes=[
            pltpu.VMEM(leaf_factor.shape, jnp.bfloat16),
            pltpu.VMEM((2, width, 2 * width), f32),
            pltpu.VMEM((2, levels * width, levels * width), f32),
            pltpu.VMEM((2 * levels * width, leaf_rows), jnp.bfloat16),
            pltpu.SemaphoreType.DMA,
        ],
        compiler_params=pltpu.CompilerParams(vmem_limit_bytes=48 * MIB),
    )(ranks, samples, order_perm.reshape(1, row_count), basis, coupling, leaf_factor)
    later = pl.pallas_call(
        functools.partial(tree_kernel, levels, width, leaf_rows),
        name="tree_part",
        out_shape=jax.ShapeDtypeStruct((steps * width, cols), f32),
        in_specs=[smem, vmem, vmem, vmem],
        out_specs=vmem,
        scratch_shapes=[
            pltpu.VMEM((max(steps - 1, 1), pairs, width, 2 * width), f32),
            pltpu.VMEM((steps, pairs, width, 2 * width), f32),
            pltpu.VMEM((max(steps - 1, 1), chunks, steps * width, chunk), f32),
            pltpu.VMEM((steps, chunks, steps * width, chunk), f32),
            pltpu.VMEM((2 * steps - 1, width, 2 * width), f32),
            pltpu.SemaphoreType.DMA((steps,)),
            pltpu.SemaphoreType.DMA((steps,)),
            pltpu.SemaphoreType.DMA((steps, chunks)),
            pltpu.SemaphoreType.DMA((steps, chunks)),
        ],
        compiler_params=pltpu.CompilerParams(
            collective_id=0, has_side_effects=True, vmem_limit_bytes=48 * MIB
        ),
    )(ranks, grams, proj, coupling)
    tile = leaf_rows // 2
    per_leaf = leaf_rows // tile
    return pl.pallas_call(
        final_kernel,
        name="final_part",
        grid=(row_count // tile,),
        out_shape=jax.ShapeDtypeStruct((cols, row_count), f32),
        in_specs=[
            pl.BlockSpec((cols, leaf_rows), lambda j: (0, j // per_leaf)),
            pl.BlockSpec((1, leaf_rows, tile), lambda j: (j // per_leaf, 0, j % per_leaf)),
            pl.BlockSpec((levels * width, tile), lambda j: (0, j)),
            pl.BlockSpec((1, width, cols), lambda j: (j // per_leaf, 0, 0)),
            pl.BlockSpec((steps * width, cols), lambda j: (0, 0)),
        ],
        out_specs=pl.BlockSpec((cols, tile), lambda j: (0, j)),
        compiler_params=pltpu.CompilerParams(vmem_limit_bytes=48 * MIB),
    )(permuted, leaf_factor, basis, first, later)


def solution(mesh):
    in_specs = (
        P("cols", "leaf"),
        P("leaf"),
        P("leaf", None, None),
        P(None, None, "leaf"),
        P(None, "leaf", None, None),
        P(),
    )
    out_specs = P("cols", "leaf")
    return jax.shard_map(local, mesh=mesh, in_specs=in_specs, out_specs=out_specs, check_vma=False)
```

```python
import functools
import math

import jax
import jax.numpy as jnp
from jax import lax
from jax.experimental import pallas as pl
from jax.experimental.pallas import tpu as pltpu
from jax.sharding import PartitionSpec as P

HIGH = lax.Precision.HIGHEST
MIB = 1024 * 1024
BLOCK = 256
PIVOTS = 8


def dot_high(a, b, contract=((1,), (0,))):
    return lax.dot_general(
        a, b, (contract, ((), ())), precision=HIGH, preferred_element_type=jnp.float32
    )


def dot_bf16(a, b, contract=((1,), (0,))):
    return lax.dot_general(a, b, (contract, ((), ())), preferred_element_type=jnp.float32)


def split(values):
    high = values.astype(jnp.bfloat16)
    return high, (values - high.astype(jnp.float32)).astype(jnp.bfloat16)


def mask(rank_value, rank_width, scale, axis):
    shape = (1, rank_width) if axis else (rank_width, 1)
    return jnp.where(lax.broadcasted_iota(jnp.int32, shape, axis) < rank_value, scale, 0.0)


def place_system(table, slot, link, gram):
    width = link.shape[0]
    rows = lax.broadcasted_iota(jnp.int32, (width, width), 0)
    eye = (rows == lax.broadcasted_iota(jnp.int32, (width, width), 1)).astype(jnp.float32)
    system = eye + dot_high(dot_high(link, gram), link, ((1,), (1,)))
    table[slot, :, :width] = system
    table[slot, :, width:] = link


def eliminate(table, slots, block):
    width, span = table.shape[1:]
    rows = lax.broadcasted_iota(jnp.int32, (PIVOTS, span), 0)
    place = pl.ds(pl.multiple_of(block * PIVOTS, PIVOTS), PIVOTS)
    whole = [table[slot] for slot in slots]
    panels = [table[slot, place, :] for slot in slots]
    for pivot in range(PIVOTS):
        for index, panel in enumerate(panels):
            column = panel[:, pivot:pivot + 1]
            row = panel[pivot:pivot + 1, :] * (1.0 / column[pivot:pivot + 1])
            panels[index] = jnp.where(rows == pivot, row, panel - column * row)
    new = [now - dot_high(now[:, :PIVOTS], panel) for now, panel in zip(whole, panels)]
    for slot, now, panel in zip(slots, new, panels):
        table[slot] = pltpu.roll(now, span - PIVOTS, 1)
        table[slot, place, :] = pltpu.roll(panel, span - PIVOTS, 1)


def pair_order(levels):
    return [(l, m) for m in range(1, levels) for l in range(m, levels)]


def tree_kernel(levels, width, ranks, samples_hbm, order_hbm, basis_hbm, coupling_hbm, leaf_hbm,
                permuted, first_out, update_out,
                samples, order, basis, coupling, leaf, local_grams, weights, first_table,
                gram_first, gram_sum, gram_recv, proj_first, proj_sum, proj_recv, table,
                fetch_sem, gram_send_sem, gram_recv_sem, proj_send_sem, proj_recv_sem):
    device = lax.axis_index("leaf")
    steps = levels - 1
    chunks, _, chunk = proj_first.shape
    pair_list = pair_order(levels)
    pairs = gram_first.shape[0]
    row_count = samples.shape[1]
    half = row_count // 2
    height = levels * width

    fetches = [
        pltpu.make_async_copy(source, target, fetch_sem.at[index])
        for index, (source, target) in enumerate((
            (basis_hbm, basis), (coupling_hbm, coupling), (order_hbm, order),
            (samples_hbm, samples), (leaf_hbm, leaf),
        ))
    ]
    for fetch in fetches:
        fetch.start()

    def partner(step):
        stride = 2 ** (step - 1)
        return device + stride * (1 - 2 * (device // stride % 2))

    barrier = pltpu.get_barrier_semaphore()
    for step in range(1, levels):
        pl.semaphore_signal(
            barrier, inc=1, device_id={"leaf": partner(step)},
            device_id_type=pl.DeviceIdType.MESH,
        )

    def gram_own(step):
        return gram_first if step == 1 else gram_sum.at[step - 2]

    def proj_own(step, index):
        return proj_first.at[index] if step == 1 else proj_sum.at[step - 2, index]

    def send_gram(step):
        first = pair_list.index((step, step)) // 2
        kept = pl.ds(first, pairs - first)
        return pltpu.make_async_remote_copy(
            src_ref=gram_own(step).at[kept],
            dst_ref=gram_recv.at[step - 1, kept],
            send_sem=gram_send_sem.at[step - 1],
            recv_sem=gram_recv_sem.at[step - 1],
            device_id={"leaf": partner(step)},
            device_id_type=pl.DeviceIdType.MESH,
        )

    def send_proj(step, index):
        kept = pl.ds((step - 1) * width, (levels - step) * width)
        return pltpu.make_async_remote_copy(
            src_ref=proj_own(step, index).at[kept],
            dst_ref=proj_recv.at[step - 1, index, kept],
            send_sem=proj_send_sem.at[step - 1, index],
            recv_sem=proj_recv_sem.at[step - 1, index],
            device_id={"leaf": partner(step)},
            device_id_type=pl.DeviceIdType.MESH,
        )

    def block(ref, pair):
        index = pair_list.index(pair)
        return ref[index // 2, :, pl.ds(index % 2 * width, width)]

    fetches[0].wait()
    for side in range(2):
        part = basis[:, side * half:(side + 1) * half]
        local_grams[side] = dot_bf16(part, part, ((1,), (1,)))
    for index, (l, m) in enumerate(pair_list):
        rows, cols = pl.ds(l * width, width), pl.ds(m * width, width)
        gram_first[index // 2, :, pl.ds(index % 2 * width, width)] = (
            local_grams[0, rows, cols] + local_grams[1, rows, cols]
        )
    if len(pair_list) % 2:
        gram_first[pairs - 1, :, pl.ds(width, width)] = jnp.zeros((width, width), jnp.float32)
    pl.semaphore_wait(barrier, steps)
    gram_copies = [send_gram(1)]
    gram_copies[0].start()

    scale = 1.0 / math.sqrt(half)
    rank = [ranks[0, 2 * device], ranks[0, 2 * device + 1]]
    fetches[1].wait()
    link = coupling[0, 0]
    links = [link, link.T]
    for side in range(2):
        scaled = links[side] * mask(rank[1 - side], width, scale, 1)
        place_system(first_table, side, scaled, local_grams[1 - side, :width, :width])

    blocks = row_count // BLOCK
    per_block = width // PIVOTS // blocks

    def permute(now, carry):
        cols = pl.ds(pl.multiple_of(now * BLOCK, BLOCK), BLOCK)
        source = order[:, cols] - device * row_count
        picks = lax.broadcasted_iota(jnp.int32, (row_count, BLOCK), 0) == source
        picks = picks.astype(jnp.float32).astype(jnp.bfloat16)
        permuted[:, cols] = dot_bf16(samples[...], picks).astype(jnp.bfloat16)
        for step in range(per_block):
            eliminate(first_table, range(2), now * per_block + step)
        return carry

    fetches[2].wait()
    fetches[3].wait()
    masks = {}
    for step in range(1, levels):
        lax.fori_loop(blocks * (step - 1) // steps, blocks * step // steps, permute, 0)
        gram_copies[step - 1].wait_recv()
        first = pair_list.index((step, step)) // 2
        if step < steps:
            kept = pl.ds(first, pairs - first)
            gram_sum[step - 1, kept] = gram_own(step)[kept] + gram_recv[step - 1, kept]
            gram_copies.append(send_gram(step + 1))
            gram_copies[step].start()
        scale = 1.0 / math.sqrt(half * 2 ** step)
        stride = 2 ** (step - 1)
        child = device // stride
        second = child % 2
        sibling = child + 1 - 2 * second
        rank_own = ranks[step, child * 2 ** step]
        rank_other = ranks[step, sibling * 2 ** step]
        masks[step] = (mask(rank_own, width, scale, 0), mask(rank_other, width, scale, 0))
        link = coupling[step, 0]
        link_own = jnp.where(second == 1, link.T, link)
        scaled = link_own * mask(rank_other, width, scale, 1)
        place_system(table, 2 * step - 2, scaled, block(gram_recv.at[step - 1], (step, step)))
        if step < steps:
            scaled = link_own.T * mask(rank_own, width, scale, 1)
            place_system(table, 2 * step - 1, scaled, block(gram_own(step), (step, step)))

    fetches[4].wait()
    projs = []
    for side in range(2):
        cols = slice(side * half, (side + 1) * half)
        high, low = split(dot_bf16(basis[:, cols], leaf[side], ((1,), (1,))))
        weights[:height] = high
        weights[height:] = low
        both = dot_bf16(weights[...], permuted[:, cols], ((1,), (1,)))
        projs.append(both[:height] + both[height:])
    later = projs[0][width:] + projs[1][width:]
    scale = 1.0 / math.sqrt(half)
    for side in range(2):
        solved = first_table[side, :, :width] * mask(rank[side], width, scale, 0)
        update = dot_high(solved, projs[1 - side][:width])
        first_out[side] = update
        later = later - dot_high(local_grams[side, width:, :width], update)
    proj_copies = {}
    for index in range(chunks):
        proj_first[index] = later[:, index * chunk:(index + 1) * chunk]
        proj_copies[1, index] = send_proj(1, index)
        proj_copies[1, index].start()

    def pivot_step(pivot, carry):
        eliminate(table, range(2 * steps - 1), pivot)
        return carry

    lax.fori_loop(0, width // PIVOTS, pivot_step, 0)

    for step in range(1, levels):
        base = (step - 1) * width
        solved_own = table[2 * step - 2, :, :width] * masks[step][0]
        if step < steps:
            solved_other = table[2 * step - 1, :, :width] * masks[step][1]
        for index in range(chunks):
            proj_copies[step, index].wait_recv()
            mine, other = proj_own(step, index), proj_recv.at[step - 1, index]
            update_own = dot_high(solved_own, other[pl.ds(base, width)])
            update_out[pl.ds(base, width), pl.ds(index * chunk, chunk)] = update_own
            if step == steps:
                continue
            update_other = dot_high(solved_other, mine[pl.ds(base, width)])
            for level in range(step + 1, levels):
                rows = pl.ds((level - 1) * width, width)
                new = mine[rows] + other[rows]
                new = new - dot_high(block(gram_own(step), (level, step)), update_own)
                new = new - dot_high(
                    block(gram_recv.at[step - 1], (level, step)), update_other
                )
                proj_sum[step - 1, index, rows] = new
            proj_copies[step + 1, index] = send_proj(step + 1, index)
            proj_copies[step + 1, index].start()
    for copy in gram_copies + list(proj_copies.values()):
        copy.wait_send()


def final_kernel(permuted, leaf, basis, first, later, out):
    update = jnp.concatenate([first[0], later[...]], axis=0)
    high, low = split(update)
    field = dot_bf16(permuted[...], leaf[0])
    field = field - dot_bf16(high, basis[...], ((0,), (0,)))
    out[...] = field - dot_bf16(low, basis[...], ((0,), (0,)))


def local(samples, order_perm, leaf_factor, bases, coupling, ranks):
    cols, row_count = samples.shape
    levels, width, _ = bases.shape
    leaf_rows = leaf_factor.shape[1]
    steps = levels - 1
    basis = bases.reshape(levels * width, row_count)
    pairs = (len(pair_order(levels)) + 1) // 2
    chunks = 4
    chunk = cols // chunks
    vmem = pl.BlockSpec(memory_space=pltpu.VMEM)
    smem = pl.BlockSpec(memory_space=pltpu.SMEM)
    f32 = jnp.float32
    hbm = pl.BlockSpec(memory_space=pltpu.MemorySpace.HBM)
    permuted, first, later = pl.pallas_call(
        functools.partial(tree_kernel, levels, width),
        name="tree_part",
        out_shape=(
            jax.ShapeDtypeStruct((cols, row_count), jnp.bfloat16),
            jax.ShapeDtypeStruct((2, width, cols), f32),
            jax.ShapeDtypeStruct((steps * width, cols), f32),
        ),
        in_specs=[smem, hbm, hbm, hbm, hbm, hbm],
        out_specs=(vmem,) * 3,
        scratch_shapes=[
            pltpu.VMEM(samples.shape, jnp.bfloat16),
            pltpu.VMEM((1, row_count), jnp.int32),
            pltpu.VMEM(basis.shape, jnp.bfloat16),
            pltpu.VMEM(coupling.shape, f32),
            pltpu.VMEM(leaf_factor.shape, jnp.bfloat16),
            pltpu.VMEM((2, levels * width, levels * width), f32),
            pltpu.VMEM((2 * levels * width, leaf_rows), jnp.bfloat16),
            pltpu.VMEM((2, width, 2 * width), f32),
            pltpu.VMEM((pairs, width, 2 * width), f32),
            pltpu.VMEM((max(steps - 1, 1), pairs, width, 2 * width), f32),
            pltpu.VMEM((steps, pairs, width, 2 * width), f32),
            pltpu.VMEM((chunks, steps * width, chunk), f32),
            pltpu.VMEM((max(steps - 1, 1), chunks, steps * width, chunk), f32),
            pltpu.VMEM((steps, chunks, steps * width, chunk), f32),
            pltpu.VMEM((2 * steps - 1, width, 2 * width), f32),
            pltpu.SemaphoreType.DMA((5,)),
            pltpu.SemaphoreType.DMA((steps,)),
            pltpu.SemaphoreType.DMA((steps,)),
            pltpu.SemaphoreType.DMA((steps, chunks)),
            pltpu.SemaphoreType.DMA((steps, chunks)),
        ],
        compiler_params=pltpu.CompilerParams(
            collective_id=0, has_side_effects=True, vmem_limit_bytes=63 * MIB
        ),
    )(ranks, samples, order_perm.reshape(1, row_count), basis, coupling, leaf_factor)
    tile = leaf_rows // 2
    per_leaf = leaf_rows // tile
    return pl.pallas_call(
        final_kernel,
        name="final_part",
        grid=(row_count // tile,),
        out_shape=jax.ShapeDtypeStruct((cols, row_count), f32),
        in_specs=[
            pl.BlockSpec((cols, leaf_rows), lambda j: (0, j // per_leaf)),
            pl.BlockSpec((1, leaf_rows, tile), lambda j: (j // per_leaf, 0, j % per_leaf)),
            pl.BlockSpec((levels * width, tile), lambda j: (0, j)),
            pl.BlockSpec((1, width, cols), lambda j: (j // per_leaf, 0, 0)),
            pl.BlockSpec((steps * width, cols), lambda j: (0, 0)),
        ],
        out_specs=pl.BlockSpec((cols, tile), lambda j: (0, j)),
        compiler_params=pltpu.CompilerParams(vmem_limit_bytes=63 * MIB),
    )(permuted, leaf_factor, basis, first, later)


def solution(mesh):
    in_specs = (
        P("cols", "leaf"),
        P("leaf"),
        P("leaf", None, None),
        P(None, None, "leaf"),
        P(None, "leaf", None, None),
        P(),
    )
    out_specs = P("cols", "leaf")
    return jax.shard_map(local, mesh=mesh, in_specs=in_specs, out_specs=out_specs, check_vma=False)
```

```python
import functools
import math

import jax
import jax.numpy as jnp
from jax import lax
from jax.experimental import pallas as pl
from jax.experimental.pallas import tpu as pltpu
from jax.sharding import PartitionSpec as P

HIGH = lax.Precision.HIGHEST
MIB = 1024 * 1024
BLOCK = 256
PIVOTS = 8


def dot_high(a, b, contract=((1,), (0,))):
    return lax.dot_general(
        a, b, (contract, ((), ())), precision=HIGH, preferred_element_type=jnp.float32
    )


def dot_bf16(a, b, contract=((1,), (0,))):
    return lax.dot_general(a, b, (contract, ((), ())), preferred_element_type=jnp.float32)


def split(values):
    high = values.astype(jnp.bfloat16)
    return high, (values - high.astype(jnp.float32)).astype(jnp.bfloat16)


def mask(rank_value, rank_width, scale, axis):
    shape = (1, rank_width) if axis else (rank_width, 1)
    return jnp.where(lax.broadcasted_iota(jnp.int32, shape, axis) < rank_value, scale, 0.0)


def place_system(table, slot, link, gram):
    width = link.shape[0]
    rows = lax.broadcasted_iota(jnp.int32, (width, width), 0)
    eye = (rows == lax.broadcasted_iota(jnp.int32, (width, width), 1)).astype(jnp.float32)
    system = eye + dot_high(dot_high(link, gram), link, ((1,), (1,)))
    table[slot, :, :width] = system
    table[slot, :, width:] = link


def eliminate(table, slots, block):
    width, span = table.shape[1:]
    rows = lax.broadcasted_iota(jnp.int32, (PIVOTS, span), 0)
    place = pl.ds(pl.multiple_of(block * PIVOTS, PIVOTS), PIVOTS)
    whole = [table[slot] for slot in slots]
    panels = [table[slot, place, :] for slot in slots]
    for pivot in range(PIVOTS):
        for index, panel in enumerate(panels):
            column = panel[:, pivot:pivot + 1]
            row = panel[pivot:pivot + 1, :] * (1.0 / column[pivot:pivot + 1])
            panels[index] = jnp.where(rows == pivot, row, panel - column * row)
    new = [now - dot_high(now[:, :PIVOTS], panel) for now, panel in zip(whole, panels)]
    for slot, now, panel in zip(slots, new, panels):
        table[slot] = pltpu.roll(now, span - PIVOTS, 1)
        table[slot, place, :] = pltpu.roll(panel, span - PIVOTS, 1)


def pair_order(levels):
    return [(l, m) for m in range(1, levels) for l in range(m, levels)]


def tree_kernel(levels, width, ranks, samples_hbm, order_hbm, basis_hbm, coupling_hbm, leaf_hbm,
                field_hbm, first_out, update_out,
                field, permuted, samples, order, basis, coupling, leaf, local_grams, weights, first_table,
                gram_first, gram_sum, gram_recv, proj_first, proj_sum, proj_recv, table,
                fetch_sem, field_sem, gram_send_sem, gram_recv_sem, proj_send_sem, proj_recv_sem):
    device = lax.axis_index("leaf")
    steps = levels - 1
    chunks, _, chunk = proj_first.shape
    pair_list = pair_order(levels)
    pairs = gram_first.shape[0]
    row_count = samples.shape[1]
    half = row_count // 2
    height = levels * width

    fetches = [
        pltpu.make_async_copy(source, target, fetch_sem.at[index])
        for index, (source, target) in enumerate((
            (basis_hbm, basis), (coupling_hbm, coupling), (order_hbm, order),
            (samples_hbm, samples), (leaf_hbm, leaf),
        ))
    ]
    for fetch in fetches:
        fetch.start()

    def partner(step):
        stride = 2 ** (step - 1)
        return device + stride * (1 - 2 * (device // stride % 2))

    barrier = pltpu.get_barrier_semaphore()
    for step in range(1, levels):
        pl.semaphore_signal(
            barrier, inc=1, device_id={"leaf": partner(step)},
            device_id_type=pl.DeviceIdType.MESH,
        )

    def gram_own(step):
        return gram_first if step == 1 else gram_sum.at[step - 2]

    def proj_own(step, index):
        return proj_first.at[index] if step == 1 else proj_sum.at[step - 2, index]

    def send_gram(step):
        first = pair_list.index((step, step)) // 2
        kept = pl.ds(first, pairs - first)
        return pltpu.make_async_remote_copy(
            src_ref=gram_own(step).at[kept],
            dst_ref=gram_recv.at[step - 1, kept],
            send_sem=gram_send_sem.at[step - 1],
            recv_sem=gram_recv_sem.at[step - 1],
            device_id={"leaf": partner(step)},
            device_id_type=pl.DeviceIdType.MESH,
        )

    def send_proj(step, index):
        kept = pl.ds((step - 1) * width, (levels - step) * width)
        return pltpu.make_async_remote_copy(
            src_ref=proj_own(step, index).at[kept],
            dst_ref=proj_recv.at[step - 1, index, kept],
            send_sem=proj_send_sem.at[step - 1, index],
            recv_sem=proj_recv_sem.at[step - 1, index],
            device_id={"leaf": partner(step)},
            device_id_type=pl.DeviceIdType.MESH,
        )

    def block(ref, pair):
        index = pair_list.index(pair)
        return ref[index // 2, :, pl.ds(index % 2 * width, width)]

    fetches[0].wait()
    for side in range(2):
        part = basis[:, side * half:(side + 1) * half]
        local_grams[side] = dot_bf16(part, part, ((1,), (1,)))
    for index, (l, m) in enumerate(pair_list):
        rows, cols = pl.ds(l * width, width), pl.ds(m * width, width)
        gram_first[index // 2, :, pl.ds(index % 2 * width, width)] = (
            local_grams[0, rows, cols] + local_grams[1, rows, cols]
        )
    if len(pair_list) % 2:
        gram_first[pairs - 1, :, pl.ds(width, width)] = jnp.zeros((width, width), jnp.float32)
    pl.semaphore_wait(barrier, steps)
    gram_copies = [send_gram(1)]
    gram_copies[0].start()

    scale = 1.0 / math.sqrt(half)
    rank = [ranks[0, 2 * device], ranks[0, 2 * device + 1]]
    fetches[1].wait()
    link = coupling[0, 0]
    links = [link, link.T]
    for side in range(2):
        scaled = links[side] * mask(rank[1 - side], width, scale, 1)
        place_system(first_table, side, scaled, local_grams[1 - side, :width, :width])

    blocks = row_count // BLOCK
    per_block = width // PIVOTS // blocks

    def permute(now, carry):
        cols = pl.ds(pl.multiple_of(now * BLOCK, BLOCK), BLOCK)
        source = order[:, cols] - device * row_count
        picks = lax.broadcasted_iota(jnp.int32, (row_count, BLOCK), 0) == source
        picks = picks.astype(jnp.float32).astype(jnp.bfloat16)
        permuted[:, cols] = dot_bf16(samples[...], picks).astype(jnp.bfloat16)
        for step in range(per_block):
            eliminate(first_table, range(2), now * per_block + step)
        return carry

    fetches[2].wait()
    fetches[3].wait()
    masks = {}
    for step in range(1, levels):
        lax.fori_loop(blocks * (step - 1) // steps, blocks * step // steps, permute, 0)
        gram_copies[step - 1].wait_recv()
        first = pair_list.index((step, step)) // 2
        if step < steps:
            kept = pl.ds(first, pairs - first)
            gram_sum[step - 1, kept] = gram_own(step)[kept] + gram_recv[step - 1, kept]
            gram_copies.append(send_gram(step + 1))
            gram_copies[step].start()
        scale = 1.0 / math.sqrt(half * 2 ** step)
        stride = 2 ** (step - 1)
        child = device // stride
        second = child % 2
        sibling = child + 1 - 2 * second
        rank_own = ranks[step, child * 2 ** step]
        rank_other = ranks[step, sibling * 2 ** step]
        masks[step] = (mask(rank_own, width, scale, 0), mask(rank_other, width, scale, 0))
        link = coupling[step, 0]
        link_own = jnp.where(second == 1, link.T, link)
        scaled = link_own * mask(rank_other, width, scale, 1)
        place_system(table, 2 * step - 2, scaled, block(gram_recv.at[step - 1], (step, step)))
        if step < steps:
            scaled = link_own.T * mask(rank_own, width, scale, 1)
            place_system(table, 2 * step - 1, scaled, block(gram_own(step), (step, step)))

    fetches[4].wait()
    projs = []
    for side in range(2):
        cols = slice(side * half, (side + 1) * half)
        high, low = split(dot_bf16(basis[:, cols], leaf[side], ((1,), (1,))))
        weights[:height] = high
        weights[height:] = low
        both = dot_bf16(weights[...], permuted[:, cols], ((1,), (1,)))
        projs.append(both[:height] + both[height:])
    later = projs[0][width:] + projs[1][width:]
    scale = 1.0 / math.sqrt(half)
    for side in range(2):
        solved = first_table[side, :, :width] * mask(rank[side], width, scale, 0)
        update = dot_high(solved, projs[1 - side][:width])
        first_out[side] = update
        later = later - dot_high(local_grams[side, width:, :width], update)
    proj_copies = {}
    for index in range(chunks):
        proj_first[index] = later[:, index * chunk:(index + 1) * chunk]
        proj_copies[1, index] = send_proj(1, index)
        proj_copies[1, index].start()

    def pivot_step(pivot, carry):
        side, place = pivot // (turns // 2), pivot % (turns // 2)
        rows = pl.ds(pl.multiple_of(side * half, half), half)
        cols = pl.ds(pl.multiple_of(place * tile, tile), tile)
        target = pl.ds(pl.multiple_of(pivot * tile, tile), tile)
        field[:, target] = dot_bf16(permuted[:, rows], leaf[side, :, cols])
        eliminate(table, range(2 * steps - 1), pivot)
        return carry

    turns = width // PIVOTS
    tile = row_count // turns
    lax.fori_loop(0, turns, pivot_step, 0)
    field_copy = pltpu.make_async_copy(field, field_hbm, field_sem)
    field_copy.start()

    for step in range(1, levels):
        base = (step - 1) * width
        solved_own = table[2 * step - 2, :, :width] * masks[step][0]
        if step < steps:
            solved_other = table[2 * step - 1, :, :width] * masks[step][1]
        for index in range(chunks):
            proj_copies[step, index].wait_recv()
            mine, other = proj_own(step, index), proj_recv.at[step - 1, index]
            update_own = dot_high(solved_own, other[pl.ds(base, width)])
            update_out[pl.ds(base, width), pl.ds(index * chunk, chunk)] = update_own
            if step == steps:
                continue
            update_other = dot_high(solved_other, mine[pl.ds(base, width)])
            for level in range(step + 1, levels):
                rows = pl.ds((level - 1) * width, width)
                new = mine[rows] + other[rows]
                new = new - dot_high(block(gram_own(step), (level, step)), update_own)
                new = new - dot_high(
                    block(gram_recv.at[step - 1], (level, step)), update_other
                )
                proj_sum[step - 1, index, rows] = new
            proj_copies[step + 1, index] = send_proj(step + 1, index)
            proj_copies[step + 1, index].start()
    for copy in gram_copies + list(proj_copies.values()):
        copy.wait_send()
    field_copy.wait()


def final_kernel(field, basis, first, later, out):
    update = jnp.concatenate([first[0], later[...]], axis=0)
    high, low = split(update)
    both = dot_bf16(high, basis[...], ((0,), (0,))) + dot_bf16(low, basis[...], ((0,), (0,)))
    out[...] = field[...] - both


def local(samples, order_perm, leaf_factor, bases, coupling, ranks):
    cols, row_count = samples.shape
    levels, width, _ = bases.shape
    leaf_rows = leaf_factor.shape[1]
    steps = levels - 1
    basis = bases.reshape(levels * width, row_count)
    pairs = (len(pair_order(levels)) + 1) // 2
    chunks = 4
    chunk = cols // chunks
    vmem = pl.BlockSpec(memory_space=pltpu.VMEM)
    smem = pl.BlockSpec(memory_space=pltpu.SMEM)
    f32 = jnp.float32
    hbm = pl.BlockSpec(memory_space=pltpu.MemorySpace.HBM)
    field, first, later = pl.pallas_call(
        functools.partial(tree_kernel, levels, width),
        name="tree_part",
        out_shape=(
            jax.ShapeDtypeStruct((cols, row_count), f32),
            jax.ShapeDtypeStruct((2, width, cols), f32),
            jax.ShapeDtypeStruct((steps * width, cols), f32),
        ),
        in_specs=[smem, hbm, hbm, hbm, hbm, hbm],
        out_specs=(hbm, vmem, vmem),
        scratch_shapes=[
            pltpu.VMEM(samples.shape, f32),
            pltpu.VMEM(samples.shape, jnp.bfloat16),
            pltpu.VMEM(samples.shape, jnp.bfloat16),
            pltpu.VMEM((1, row_count), jnp.int32),
            pltpu.VMEM(basis.shape, jnp.bfloat16),
            pltpu.VMEM(coupling.shape, f32),
            pltpu.VMEM(leaf_factor.shape, jnp.bfloat16),
            pltpu.VMEM((2, levels * width, levels * width), f32),
            pltpu.VMEM((2 * levels * width, leaf_rows), jnp.bfloat16),
            pltpu.VMEM((2, width, 2 * width), f32),
            pltpu.VMEM((pairs, width, 2 * width), f32),
            pltpu.VMEM((max(steps - 1, 1), pairs, width, 2 * width), f32),
            pltpu.VMEM((steps, pairs, width, 2 * width), f32),
            pltpu.VMEM((chunks, steps * width, chunk), f32),
            pltpu.VMEM((max(steps - 1, 1), chunks, steps * width, chunk), f32),
            pltpu.VMEM((steps, chunks, steps * width, chunk), f32),
            pltpu.VMEM((2 * steps - 1, width, 2 * width), f32),
            pltpu.SemaphoreType.DMA((5,)),
            pltpu.SemaphoreType.DMA,
            pltpu.SemaphoreType.DMA((steps,)),
            pltpu.SemaphoreType.DMA((steps,)),
            pltpu.SemaphoreType.DMA((steps, chunks)),
            pltpu.SemaphoreType.DMA((steps, chunks)),
        ],
        compiler_params=pltpu.CompilerParams(
            collective_id=0, has_side_effects=True, vmem_limit_bytes=63 * MIB
        ),
    )(ranks, samples, order_perm.reshape(1, row_count), basis, coupling, leaf_factor)
    tile = leaf_rows // 2
    per_leaf = leaf_rows // tile
    return pl.pallas_call(
        final_kernel,
        name="final_part",
        grid=(row_count // tile,),
        out_shape=jax.ShapeDtypeStruct((cols, row_count), f32),
        in_specs=[
            pl.BlockSpec((cols, tile), lambda j: (0, j)),
            pl.BlockSpec((levels * width, tile), lambda j: (0, j)),
            pl.BlockSpec((1, width, cols), lambda j: (j // per_leaf, 0, 0)),
            pl.BlockSpec((steps * width, cols), lambda j: (0, 0)),
        ],
        out_specs=pl.BlockSpec((cols, tile), lambda j: (0, j)),
        compiler_params=pltpu.CompilerParams(vmem_limit_bytes=63 * MIB),
    )(field, basis, first, later)


def solution(mesh):
    in_specs = (
        P("cols", "leaf"),
        P("leaf"),
        P("leaf", None, None),
        P(None, None, "leaf"),
        P(None, "leaf", None, None),
        P(),
    )
    out_specs = P("cols", "leaf")
    return jax.shard_map(local, mesh=mesh, in_specs=in_specs, out_specs=out_specs, check_vma=False)
```
